128 devices in a mesh: step: 2 (over core), tile: 64 (over z, y, x).
Axes of the slice: x: 4, y: 4, z: 4, core: 2. Of those that a mesh axis runs over, the one named last changes fastest.
Arguments:
- latents: float32 [2, 8192, 3072], P('step', 'tile'), may hold values from -6 to 6
- start: float32 [8192, 3072], P('tile'), may hold values from -6 to 6
- cached_velocity: float32 [2, 8192, 3072], P('step', 'tile'), may hold values from -4 to 4
- shift: float32 [2, 3072], P('step'), may hold values from -3 to 3
- scale: float32 [2, 3072], P('step'), may hold values from -3 to 3
- gate: float32 [2, 3072], P('step'), may hold values from -10 to 10
- step_sizes: float32 [2], P('step'), may hold values from 0.1 to 0.5
- converged: int32 [2, 64], P(None, 'tile'), may hold values from 0 to 1, as said below
- neighbours: int32 [64, 4], P('tile'), may hold values from 0 to 1, as said below
- w_qkv: bfloat16 [3, 3072, 2048], P(None, None, 'step'), may hold values from -0.109375 to 0.109375
- q_gain: float32 [128], replicated, may hold values from 0.1 to 1.9
- k_gain: float32 [128], replicated, may hold values from 0.1 to 1.9
- w_out: bfloat16 [2048, 3072], P('step', 'tile'), may hold values from -0.5 to 0.5
Outputs:
- updated: float32 [2, 8192, 3072], P('step', 'tile')
- velocity: float32 [2, 8192, 3072], P('step', 'tile')
The draws below stay inside these ranges and needn't reach their ends.
Inputs may be any that keep to these rules, and one draw needn't show every extreme that they name: For each tile the converged steps are the first ones of the window, at most 1 of them. `neighbours`: an entry is 0 wherever the grid of 16 rows of 4 tiles has no neighbour that way.
All inputs are finite; a program needn't handle non-finite values.
Results may differ from the reference program's by a relative error of at most 0.008.
Values may be sent and summed in bfloat16 or wider, within the bound.
No kernel may reach another device: no remote copies, remote signals or barrier semaphores. Data moves between devices by JAX's collectives and lax.ppermute only.
A program may use at most 128 MiB of HBM per device.

```python
import math
import jax
import jax.numpy as jnp
from jax import lax

D = 3072
HEADS = 16
HD = 128
GRID_COLS = 4
TILE_TOK = 128
STEPS = 2
TOKENS = 8192
N_TILE = 64


def draw_converged(key, part):
    counts = jax.random.randint(key, (N_TILE,), 0, STEPS // 2 + 1)
    positions = jnp.arange(STEPS)[:, None]
    return (positions < counts[None, :]).astype(jnp.int32)


def draw_neighbours(key, part):
    picks = jax.random.randint(key, (N_TILE, 4), 0, 4) > 0
    tiles = jnp.arange(N_TILE)
    column = tiles % GRID_COLS
    row_index = tiles // GRID_COLS
    row_count = N_TILE // GRID_COLS
    valid = jnp.stack([column > 0, column < GRID_COLS - 1, row_index > 0, row_index < row_count - 1], axis=1)
    return (picks & valid).astype(jnp.int32)


def shard_levels(stream_key, shape, pieces, low, top_value):
    level, own = 1.0, jax.random.fold_in(stream_key, 6)
    for dim, shards_of in pieces:
        draws = jnp.exp(jax.random.uniform(jax.random.fold_in(own, dim), (shards_of,), jnp.float32, low / len(pieces), top_value / len(pieces)))
        level = level * jnp.repeat(draws, shape[dim] // shards_of).reshape([-1 if axis == dim else 1 for axis in range(len(shape))])
    return level


def centred(stream_key, dims, scale, reach, split=(), held_as=jnp.bfloat16):
    factor_of = shard_levels(stream_key, dims, split, -0.22, 0.18) if split else 1.0
    result = jax.random.normal(stream_key, dims, jnp.float32) * scale * factor_of
    return jnp.minimum(jnp.maximum(result, -reach), reach).astype(held_as)


def setup_inputs(seed: int = 0) -> dict:
    keys = jax.random.split(jax.random.key(seed), 14)
    return {
        "latents": centred(keys[0], (STEPS, TOKENS, D), 1.0, 6.0, ((0, 2), (1, 64)), jnp.float32),
        "start": centred(keys[1], (TOKENS, D), 1.0, 6.0, ((0, 64),), jnp.float32),
        "cached_velocity": centred(keys[2], (STEPS, TOKENS, D), 0.5, 4.0, ((0, 2), (1, 64)), jnp.float32),
        "shift": centred(keys[3], (STEPS, D), 0.5, 3.0, ((0, 2),), jnp.float32),
        "scale": centred(keys[4], (STEPS, D), 0.5, 3.0, ((0, 2),), jnp.float32),
        "gate": centred(keys[5], (STEPS, D), 2.0, 10.0, ((0, 2),), jnp.float32),
        "step_sizes": jnp.clip(jnp.exp(math.log(0.5) - 1.609438 * jax.random.uniform(keys[6], (STEPS,), jnp.float32) ** shard_levels(keys[6], (STEPS,), ((0, 2),), -0.2, 0.2)), 0.1, 0.5),
        "converged": draw_converged(jax.random.fold_in(keys[13], 71), 0),
        "neighbours": draw_neighbours(jax.random.fold_in(keys[13], 71), 0),
        "w_qkv": centred(keys[9], (3, D, HEADS * HD), D ** -0.5, 0.109375, ((2, 2),)),
        "q_gain": jnp.clip(1.0 + 0.18 * jax.random.normal(keys[10], (HD,), jnp.float32), 0.1, 1.9),
        "k_gain": jnp.clip(1.0 + 0.18 * jax.random.normal(keys[11], (HD,), jnp.float32), 0.1, 1.9),
        "w_out": centred(keys[12], (HEADS * HD, D), HD ** -0.5, 0.5, ((0, 2), (1, 64))),
    }


def reference(latents, start, cached_velocity, shift, scale, gate, step_sizes, converged, neighbours, w_qkv, q_gain, k_gain, w_out):
    high = lax.Precision.HIGHEST
    key_mask = jnp.concatenate([jnp.ones((N_TILE, TILE_TOK), jnp.float32), jnp.repeat(neighbours.astype(jnp.float32), TILE_TOK, axis=1)], axis=1)
    weights_f = w_qkv.astype(jnp.float32)
    out_f = w_out.astype(jnp.float32)

    def one_step(items):
        lat, shf, scl = items
        mean = lax.optimization_barrier(jnp.mean(lat, axis=-1, keepdims=True))
        var = lax.optimization_barrier(jnp.mean(jnp.square(lat - mean), axis=-1, keepdims=True))
        normed = ((lat - mean) / jnp.sqrt(var + 1e-06) * (1.0 + scl) + shf).astype(jnp.bfloat16)
        qkv = jnp.einsum('td,cdf->ctf', normed.astype(jnp.float32), weights_f, precision=high)
        qkv = qkv.reshape(3, N_TILE, TILE_TOK, HEADS, HD)

        def rms(block, gain):
            return (block / jnp.sqrt(lax.optimization_barrier(jnp.mean(block * block, axis=-1, keepdims=True)) + 1e-06) * gain).astype(jnp.bfloat16)
        queries = rms(qkv[0], q_gain)
        keys_own = rms(qkv[1], k_gain)
        values_own = qkv[2].astype(jnp.bfloat16)

        def beside_all(block):
            return jnp.concatenate([block, jnp.roll(block, 1, axis=0), jnp.roll(block, -1, axis=0), jnp.roll(block, GRID_COLS, axis=0), jnp.roll(block, -GRID_COLS, axis=0)], axis=1)
        keys_all = beside_all(keys_own).astype(jnp.float32)
        values_all = beside_all(values_own).astype(jnp.float32)
        scores = jnp.einsum('tqhd,tkhd->thqk', queries.astype(jnp.float32), keys_all, precision=high) / jnp.sqrt(jnp.float32(HD))
        expo = jnp.exp(scores) * key_mask[:, None, None, :]
        probs = (expo / lax.optimization_barrier(jnp.sum(expo, axis=-1, keepdims=True))).astype(jnp.bfloat16)
        attended = jnp.einsum('thqk,tkhd->tqhd', probs.astype(jnp.float32), values_all, precision=high).astype(jnp.bfloat16)
        attended = attended.reshape(TOKENS, HEADS * HD)
        return jnp.dot(attended.astype(jnp.float32), out_f, precision=high)
    projected = lax.map(one_step, (latents, shift[:, None, :], scale[:, None, :]))
    frozen = jnp.repeat(converged, TILE_TOK, axis=1)[:, :, None] == 1
    velocity = jnp.where(frozen, cached_velocity, gate[:, None, :] * projected)
    terms = step_sizes[:, None, None] * velocity
    summed = jnp.cumsum(terms, axis=0)
    prefix = jnp.concatenate([jnp.zeros((1, TOKENS, D), jnp.float32), summed[:-1]], axis=0)
    updated = start[None, :, :] + prefix
    return (updated, velocity)
```

```python
import jax
import jax.numpy as jnp
from jax import lax
from jax.experimental import pallas as pl
from jax.experimental.pallas import tpu as pltpu
from jax.sharding import PartitionSpec as P

GRID_COLS = 4
SIDE = 4
TILES = SIDE**3
F32 = jnp.float32
BF16 = jnp.bfloat16
NORM_COST = 16 * 10**9
OUTPUT_COST = 8 * 10**9
LOG2E = 1.4426950408889634
STRIDES = {"z": 16, "y": 4, "x": 1}
ORDERS = ((("x", "y", "z"), ("y", "x", "z")), (("x", "z", "y"), ("y", "z", "x")))
UNITS = (16, 32)
BOTH = ("step", "tile")
SWAP = [(0, 1), (1, 0)]


def partner(place, core, second):
    if core == second:
        return place ^ 1
    return (place + 1 if place % 2 else place - 1) % SIDE


def opposite(place, core, second):
    return (place + 2) % SIDE


def along(block, dims, second, target_of=partner):
    pairs = []
    for core in range(2):
        stride = STRIDES[dims[core]]
        for tile in range(TILES):
            place = tile // stride % SIDE
            target = tile + (target_of(place, core, second) - place) * stride
            pairs.append((core * TILES + tile, core * TILES + target))
    return lax.ppermute(block, BOTH, pairs)


def four(block, dims):
    first, second = along(block, dims, 0), along(block, dims, 1)
    return jnp.concatenate([block, first, second, along(block, dims, 0, opposite)], axis=0)


def neighbour_pairs(move):
    if abs(move) == 1:
        return [(t, t // GRID_COLS * GRID_COLS + (t + move) % GRID_COLS) for t in range(TILES)]
    return [(t, (t + move) % TILES) for t in range(TILES)]


def norm_kernel(x_any, scale_any, shift_any, out_ref, x_ref, scale_ref, shift_ref, sems):
    copies = [
        pltpu.make_async_copy(source, target, sems.at[i])
        for i, (source, target) in enumerate(((x_any, x_ref), (scale_any, scale_ref), (shift_any, shift_ref)))
    ]
    for copy in copies:
        copy.start()
    for copy in copies:
        copy.wait()
    x = x_ref[...]
    mean = jnp.mean(x, axis=-1, keepdims=True)
    centred = x - mean
    var = jnp.mean(centred * centred, axis=-1, keepdims=True)
    scaled = centred * (1.0 / jnp.sqrt(var + 1e-06)) * (1.0 + scale_ref[...]) + shift_ref[...]
    out_ref[...] = scaled.astype(BF16)


def limit(mib):
    return pltpu.CompilerParams(vmem_limit_bytes=mib << 20)


def normalize(x, scale, shift):
    rows, width = x.shape
    return pl.pallas_call(
        norm_kernel,
        in_specs=[pl.BlockSpec(memory_space=pltpu.HBM)] * 3,
        out_specs=pl.BlockSpec(memory_space=pltpu.VMEM),
        out_shape=jax.ShapeDtypeStruct((rows, width), BF16),
        scratch_shapes=[
            pltpu.VMEM((rows, width), F32),
            pltpu.VMEM((1, width), F32),
            pltpu.VMEM((1, width), F32),
            pltpu.SemaphoreType.DMA((3,)),
        ],
        compiler_params=limit(8),
        cost_estimate=pl.CostEstimate(flops=NORM_COST, transcendentals=0, bytes_accessed=6 * rows * width),
    )(*(pltpu.with_memory_space_constraint(value, pltpu.HBM) for value in (x, scale, shift)))


def make_project_kernel(head, first, parts, normed_parts, span):
    def kernel(own_ref, other_ref, w_ref, gain_ref, out_ref, x_ref):
        tokens = own_ref.shape[0]
        x_ref[:tokens, :] = own_ref[...]
        x_ref[tokens:, :] = other_ref[...]
        ones = jnp.full((head, head), 1.0 / head, BF16)
        for part in range(parts):
            for at in range(0, w_ref.shape[2], span):
                acc = jnp.dot(x_ref[...], w_ref[first + part, :, at : at + span], preferred_element_type=F32)
                if part < normed_parts:
                    blocks = []
                    for h in range(span // head):
                        block = acc[:, h * head : (h + 1) * head]
                        mean = jnp.dot((block * block).astype(BF16), ones, preferred_element_type=F32)
                        blocks.append((block * lax.rsqrt(mean + 1e-06) * gain_ref[...]).astype(BF16))
                    done = jnp.concatenate(blocks, axis=1)
                else:
                    done = acc.astype(BF16)
                out_ref[part, 0, :, at : at + span] = done[:tokens]
                out_ref[part, 1, :, at : at + span] = done[tokens:]

    return kernel


def project(own, other, w_qkv, gain, first, parts, normed_parts):
    tokens, width = own.shape
    cols = w_qkv.shape[2]
    return pl.pallas_call(
        make_project_kernel(gain.shape[-1], first, parts, normed_parts, cols // 2),
        in_specs=[pl.BlockSpec(memory_space=pltpu.VMEM)] * 4,
        out_specs=pl.BlockSpec(memory_space=pltpu.VMEM),
        out_shape=jax.ShapeDtypeStruct((parts, 2, tokens, cols), BF16),
        scratch_shapes=[pltpu.VMEM((2 * tokens, width), BF16)],
        compiler_params=limit(8),
        cost_estimate=pl.CostEstimate(
            flops=4 * tokens * width * cols * parts,
            transcendentals=0,
            bytes_accessed=2 * (parts * width * cols + 2 * tokens * width),
        ),
    )(own, other, w_qkv, gain)


def make_attend_kernel(head, factor):
    def kernel(near_ref, q_ref, own_ref, a_ref, b_ref, c_ref, d_ref, out_ref):
        sources = (own_ref, a_ref, b_ref, c_ref, d_ref)
        tokens = q_ref.shape[2]
        ones = jnp.ones((tokens, head), BF16)
        masks = [None] + [near_ref[0, j].astype(F32).astype(BF16) for j in range(4)]
        counts = jnp.concatenate([ones if mask is None else ones * mask for mask in masks], axis=0)
        for s in range(q_ref.shape[1]):
            for h in range(q_ref.shape[3] // head):
                lanes = slice(h * head, (h + 1) * head)
                keys = jnp.concatenate([ref[0, s, :, lanes] for ref in sources], axis=0)
                values = jnp.concatenate(
                    [
                        ref[1, s, :, lanes] if mask is None else ref[1, s, :, lanes] * mask
                        for ref, mask in zip(sources, masks)
                    ],
                    axis=0,
                )
                scores = lax.dot_general(
                    q_ref[0, s, :, lanes], keys, (((1,), (1,)), ((), ())), preferred_element_type=F32
                )
                p = jnp.exp2(scores * (factor * LOG2E)).astype(BF16)
                both = jnp.dot(p, jnp.concatenate([values, counts], axis=1), preferred_element_type=F32)
                out_ref[s, :, lanes] = (both[:, :head] / both[:, head:]).astype(BF16)

    return kernel


def attention(near, queries, sources, head):
    _, steps, tokens, cols = queries.shape
    factor = 1.0 / float(head) ** 0.5
    return pl.pallas_call(
        make_attend_kernel(head, factor),
        in_specs=[pl.BlockSpec(memory_space=pltpu.SMEM)]
        + [pl.BlockSpec(memory_space=pltpu.VMEM)] * (1 + len(sources)),
        out_specs=pl.BlockSpec(memory_space=pltpu.VMEM),
        out_shape=jax.ShapeDtypeStruct((steps, tokens, cols), BF16),
        compiler_params=limit(8),
        cost_estimate=pl.CostEstimate(
            flops=4 * steps * tokens * 5 * tokens * cols,
            transcendentals=steps * tokens * 5 * tokens * cols // head,
            bytes_accessed=2 * 12 * steps * tokens * cols,
        ),
    )(near, queries, *sources)


def slot_place(place, core, slot):
    if slot == 0:
        return place
    if slot == 3:
        return place ^ 2
    near = place ^ 1
    far = (place + 2 * (place & 1) - 1) & (SIDE - 1)
    return jnp.where(core == slot - 1, near, far)


def make_output_kernel(shard):
    def kernel(place_ref, a_ref, *refs):
        pieces, out_ref, w_ref, sem = refs[:-3], refs[-3], refs[-2], refs[-1]
        core = place_ref[0]
        where = {"z": 1, "y": 2, "x": 3}
        for colour, orders in enumerate(ORDERS):
            unit = UNITS[colour]
            parts = []
            for level in range(3):
                first, second = orders[0][level], orders[1][level]
                place = jnp.where(core == 0, place_ref[where[first]], place_ref[where[second]])
                stride = jnp.where(core == 0, STRIDES[first], STRIDES[second])
                parts.append([slot_place(place, core, slot) * stride for slot in range(SIDE)])
            mine = pieces[:SIDE] if colour == 0 else pieces[SIDE:]
            blocks = [[(ref, at * unit) for at in range(SIDE * SIDE)] for ref in mine[: SIDE - 1]]
            count = SIDE * SIDE // len(mine[SIDE - 1 :])
            blocks.append([(ref, at * unit) for ref in mine[SIDE - 1 :] for at in range(count)])
            for slot in range(SIDE):
                for at, (ref, row) in enumerate(blocks[slot]):
                    tile = parts[2][slot] + parts[1][at // SIDE] + parts[0][at % SIDE]
                    target = pl.multiple_of(tile * shard + sum(UNITS[:colour]), 8)
                    pltpu.make_async_copy(ref.at[pl.ds(row, unit)], w_ref.at[pl.ds(target, unit)], sem).start()
        pltpu.make_async_copy(w_ref, w_ref, sem).wait()
        steps, tokens, cols = a_ref.shape
        left = a_ref[...].reshape(steps * tokens, cols)
        chunk = 512
        for at in range(0, w_ref.shape[0], chunk):
            right = w_ref[at : at + chunk, :]
            done = lax.dot_general(left, right, (((1,), (1,)), ((), ())), preferred_element_type=F32).astype(BF16)
            for s in range(steps):
                out_ref[1 - s, :, at : at + chunk] = done[s * tokens : (s + 1) * tokens]

    return kernel


def output_project(place, attended, pieces, width, shard):
    steps, tokens, cols = attended.shape
    return pl.pallas_call(
        make_output_kernel(shard),
        in_specs=[
            pl.BlockSpec(memory_space=pltpu.SMEM),
            pl.BlockSpec(memory_space=pltpu.VMEM),
        ]
        + [pl.BlockSpec(memory_space=pltpu.HBM)] * len(pieces),
        out_specs=pl.BlockSpec(memory_space=pltpu.VMEM),
        out_shape=jax.ShapeDtypeStruct((steps, tokens, width), BF16),
        scratch_shapes=[pltpu.VMEM((width, cols), BF16), pltpu.SemaphoreType.DMA],
        compiler_params=limit(16),
        cost_estimate=pl.CostEstimate(
            flops=OUTPUT_COST,
            transcendentals=0,
            bytes_accessed=2 * (cols * width + steps * tokens * (cols + width)),
        ),
    )(place, attended, *(pltpu.with_memory_space_constraint(piece, pltpu.HBM) for piece in pieces))


def make_finish_kernel(parts):
    def kernel(
        place_ref, converged_ref, terms_ref, arrived_ref, start_ref, cached_ref, gate_ref, held_ref, pace_ref,
        updated_ref, velocity_ref, buf_ref, sems,
    ):
        frozen = converged_ref[place_ref[0]] > 0
        frozen_first = converged_ref[0] > 0
        gate = gate_ref[...]
        pace = pace_ref[...]
        rows = buf_ref.shape[2]
        copies = []
        for i in range(parts):
            at = slice(i * rows, (i + 1) * rows)
            mine = terms_ref[1, at, :].astype(F32) + arrived_ref[0, at, :].astype(F32)
            buf_ref[i, 1] = jnp.where(frozen, cached_ref[at, :], gate * mine)
            theirs = terms_ref[0, at, :].astype(F32) + arrived_ref[1, at, :].astype(F32)
            prefix = jnp.where(frozen_first, held_ref[at, :].astype(F32), pace * theirs)
            buf_ref[i, 0] = start_ref[at, :] + prefix
            for j, ref in enumerate((updated_ref, velocity_ref)):
                copy = pltpu.make_async_copy(buf_ref.at[i, j], ref.at[pl.ds(i * rows, rows)], sems.at[i, j])
                copy.start()
                copies.append(copy)
        for copy in copies:
            copy.wait()

    return kernel


def finish(place, converged, terms, arrived, start, cached, gate, held, pace):
    tokens, width = start.shape
    parts = 4
    out = jax.ShapeDtypeStruct((tokens, width), F32)
    return pl.pallas_call(
        make_finish_kernel(parts),
        in_specs=[pl.BlockSpec(memory_space=pltpu.SMEM)] * 2 + [pl.BlockSpec(memory_space=pltpu.VMEM)] * 7,
        out_specs=[pl.BlockSpec(memory_space=pltpu.HBM)] * 2,
        out_shape=[out, out],
        scratch_shapes=[
            pltpu.VMEM((parts, 2, tokens // parts, width), F32),
            pltpu.SemaphoreType.DMA((parts, 2)),
        ],
        compiler_params=limit(8),
        cost_estimate=pl.CostEstimate(
            flops=8 * tokens * width, transcendentals=0, bytes_accessed=26 * tokens * width
        ),
    )(place, converged, terms, arrived, start, cached, gate, held, pace)


def start_gather(w_out):
    dims = tuple(order[0] for order in ORDERS[0])
    block = w_out.T[None]
    block = four(block, dims)
    parts, at = [], 0
    for unit in UNITS:
        parts.append(block[:, at : at + unit].reshape(SIDE * unit, -1))
        at += unit
    return parts


def finish_gather(colour, line):
    orders = ORDERS["ab".index(colour)]
    dims = tuple(order[1] for order in orders)
    plane = four(line, dims)
    dims = tuple(order[2] for order in orders)
    first, second = along(plane, dims, 0), along(plane, dims, 1)
    if colour == "a":
        return [plane, first, second, along(first, dims, 1)]
    half = plane.shape[0] // 2
    low = along(first[:half], dims, 1)
    return [plane, first, second, low, along(second[half:], dims, 0)]


def body(
    latents,
    start,
    cached_velocity,
    shift,
    scale,
    gate,
    step_sizes,
    converged,
    neighbours,
    w_qkv,
    q_gain,
    k_gain,
    w_out,
):
    _, width = latents.shape[1:]
    head = q_gain.shape[0]
    shard = w_out.shape[1]
    here = lax.axis_index("step")
    tile = lax.axis_index("tile")
    place = jnp.stack([here, tile // 16, tile // 4 % 4, tile % 4]).astype(jnp.int32)

    own = normalize(latents[0], scale, shift)
    other = lax.ppermute(own, "step", SWAP)

    lines = start_gather(w_out)
    pieces = finish_gather("a", lines[0]) + finish_gather("b", lines[1])

    pair = project(own, other, w_qkv, k_gain[None], 1, 2, 1)
    around = []
    for move in (1, -1, GRID_COLS, -GRID_COLS):
        around.append(lax.ppermute(pair, "tile", neighbour_pairs(move)))
    step_size = step_sizes[0]
    to_send = (step_size * cached_velocity[0]).astype(BF16)
    sent_cached = lax.ppermute(to_send, "step", [(0, 1)])
    sent_gate = lax.ppermute(step_size * gate, "step", [(0, 1)])
    queries = project(own, other, w_qkv, q_gain[None], 0, 1, 1)
    queries, sent_cached, sent_gate = lax.optimization_barrier((queries, sent_cached, sent_gate))
    attended = attention(neighbours, queries, [pair] + around, head)
    terms = output_project(place, attended, pieces, width, shard)

    arrived = lax.ppermute(terms, "step", SWAP)
    updated, velocity = finish(
        place, converged[:, 0], terms, arrived, start, cached_velocity[0], gate, sent_cached, sent_gate
    )
    return (updated[None], velocity[None])


def solution(mesh):
    placed = (
        P("step", "tile", None),
        P("tile", None),
        P("step", "tile", None),
        P("step", None),
        P("step", None),
        P("step", None),
        P("step"),
        P(None, "tile"),
        P("tile", None),
        P(None, None, "step"),
        P(),
        P(),
        P("step", "tile"),
    )

    return jax.shard_map(
        body,
        mesh=mesh,
        in_specs=placed,
        out_specs=(P("step", "tile", None), P("step", "tile", None)),
        check_vma=False,
    )
```

```python
import jax
import jax.numpy as jnp
from jax import lax
from jax.experimental import pallas as pl
from jax.experimental.pallas import tpu as pltpu
from jax.sharding import PartitionSpec as P

GRID_COLS = 4
SIDE = 4
TILES = SIDE**3
F32 = jnp.float32
BF16 = jnp.bfloat16
NORM_COST = 16 * 10**9
OUTPUT_COST = 8 * 10**9
LOG2E = 1.4426950408889634
STRIDES = {"z": 16, "y": 4, "x": 1}
ORDERS = ((("x", "y", "z"), ("y", "x", "z")), (("x", "z", "y"), ("y", "z", "x")))
UNITS = (16, 32)
BOTH = ("step", "tile")
SWAP = [(0, 1), (1, 0)]


def partner(place, core, second):
    if core == second:
        return place ^ 1
    return (place + 1 if place % 2 else place - 1) % SIDE


def opposite(place, core, second):
    return (place + 2) % SIDE


def along(block, dims, second, target_of=partner):
    pairs = []
    for core in range(2):
        stride = STRIDES[dims[core]]
        for tile in range(TILES):
            place = tile // stride % SIDE
            target = tile + (target_of(place, core, second) - place) * stride
            pairs.append((core * TILES + tile, core * TILES + target))
    return lax.ppermute(block, BOTH, pairs)


def four(block, dims):
    first, second = along(block, dims, 0), along(block, dims, 1)
    return jnp.concatenate([block, first, second, along(block, dims, 0, opposite)], axis=0)


def neighbour_pairs(move):
    if abs(move) == 1:
        return [(t, t // GRID_COLS * GRID_COLS + (t + move) % GRID_COLS) for t in range(TILES)]
    return [(t, (t + move) % TILES) for t in range(TILES)]


def norm_kernel(x_any, scale_any, shift_any, out_ref, x_ref, scale_ref, shift_ref, sems):
    copies = [
        pltpu.make_async_copy(source, target, sems.at[i])
        for i, (source, target) in enumerate(((x_any, x_ref), (scale_any, scale_ref), (shift_any, shift_ref)))
    ]
    for copy in copies:
        copy.start()
    for copy in copies:
        copy.wait()
    x = x_ref[...]
    mean = jnp.mean(x, axis=-1, keepdims=True)
    centred = x - mean
    var = jnp.mean(centred * centred, axis=-1, keepdims=True)
    scaled = centred * (1.0 / jnp.sqrt(var + 1e-06)) * (1.0 + scale_ref[...]) + shift_ref[...]
    out_ref[...] = scaled.astype(BF16)


def limit(mib):
    return pltpu.CompilerParams(vmem_limit_bytes=mib << 20)


def normalize(x, scale, shift):
    rows, width = x.shape
    return pl.pallas_call(
        norm_kernel,
        in_specs=[pl.BlockSpec(memory_space=pltpu.HBM)] * 3,
        out_specs=pl.BlockSpec(memory_space=pltpu.VMEM),
        out_shape=jax.ShapeDtypeStruct((rows, width), BF16),
        scratch_shapes=[
            pltpu.VMEM((rows, width), F32),
            pltpu.VMEM((1, width), F32),
            pltpu.VMEM((1, width), F32),
            pltpu.SemaphoreType.DMA((3,)),
        ],
        compiler_params=limit(8),
        cost_estimate=pl.CostEstimate(flops=NORM_COST, transcendentals=0, bytes_accessed=6 * rows * width),
    )(*(pltpu.with_memory_space_constraint(value, pltpu.HBM) for value in (x, scale, shift)))


def make_project_kernel(head, first, parts, normed_parts, span):
    def kernel(own_ref, other_ref, w_ref, gain_ref, out_ref, x_ref):
        tokens = own_ref.shape[0]
        x_ref[:tokens, :] = own_ref[...]
        x_ref[tokens:, :] = other_ref[...]
        ones = jnp.full((head, head), 1.0 / head, BF16)
        for part in range(parts):
            for at in range(0, w_ref.shape[2], span):
                acc = jnp.dot(x_ref[...], w_ref[first + part, :, at : at + span], preferred_element_type=F32)
                if part < normed_parts:
                    blocks = []
                    for h in range(span // head):
                        block = acc[:, h * head : (h + 1) * head]
                        mean = jnp.dot((block * block).astype(BF16), ones, preferred_element_type=F32)
                        blocks.append((block * lax.rsqrt(mean + 1e-06) * gain_ref[...]).astype(BF16))
                    done = jnp.concatenate(blocks, axis=1)
                else:
                    done = acc.astype(BF16)
                out_ref[part, 0, :, at : at + span] = done[:tokens]
                out_ref[part, 1, :, at : at + span] = done[tokens:]

    return kernel


def project(own, other, w_qkv, gain, first, parts, normed_parts):
    tokens, width = own.shape
    cols = w_qkv.shape[2]
    return pl.pallas_call(
        make_project_kernel(gain.shape[-1], first, parts, normed_parts, cols // 2),
        in_specs=[pl.BlockSpec(memory_space=pltpu.VMEM)] * 4,
        out_specs=pl.BlockSpec(memory_space=pltpu.VMEM),
        out_shape=jax.ShapeDtypeStruct((parts, 2, tokens, cols), BF16),
        scratch_shapes=[pltpu.VMEM((2 * tokens, width), BF16)],
        compiler_params=limit(8),
        cost_estimate=pl.CostEstimate(
            flops=4 * tokens * width * cols * parts,
            transcendentals=0,
            bytes_accessed=2 * (parts * width * cols + 2 * tokens * width),
        ),
    )(own, other, w_qkv, gain)


def make_attend_kernel(head, factor):
    def kernel(near_ref, q_ref, own_ref, a_ref, b_ref, c_ref, d_ref, out_ref):
        sources = (own_ref, a_ref, b_ref, c_ref, d_ref)
        tokens = q_ref.shape[2]
        ones = jnp.ones((tokens, head), BF16)
        masks = [None] + [near_ref[0, j].astype(F32).astype(BF16) for j in range(4)]
        counts = jnp.concatenate([ones if mask is None else ones * mask for mask in masks], axis=0)
        for s in range(q_ref.shape[1]):
            for h in range(q_ref.shape[3] // head):
                lanes = slice(h * head, (h + 1) * head)
                keys = jnp.concatenate([ref[0, s, :, lanes] for ref in sources], axis=0)
                values = jnp.concatenate(
                    [
                        ref[1, s, :, lanes] if mask is None else ref[1, s, :, lanes] * mask
                        for ref, mask in zip(sources, masks)
                    ],
                    axis=0,
                )
                scores = lax.dot_general(
                    q_ref[0, s, :, lanes], keys, (((1,), (1,)), ((), ())), preferred_element_type=F32
                )
                p = jnp.exp2(scores * (factor * LOG2E)).astype(BF16)
                both = jnp.dot(p, jnp.concatenate([values, counts], axis=1), preferred_element_type=F32)
                out_ref[s, :, lanes] = (both[:, :head] / both[:, head:]).astype(BF16)

    return kernel


def attention(near, queries, sources, head):
    _, steps, tokens, cols = queries.shape
    factor = 1.0 / float(head) ** 0.5
    return pl.pallas_call(
        make_attend_kernel(head, factor),
        in_specs=[pl.BlockSpec(memory_space=pltpu.SMEM)]
        + [pl.BlockSpec(memory_space=pltpu.VMEM)] * (1 + len(sources)),
        out_specs=pl.BlockSpec(memory_space=pltpu.VMEM),
        out_shape=jax.ShapeDtypeStruct((steps, tokens, cols), BF16),
        compiler_params=limit(8),
        cost_estimate=pl.CostEstimate(
            flops=4 * steps * tokens * 5 * tokens * cols,
            transcendentals=steps * tokens * 5 * tokens * cols // head,
            bytes_accessed=2 * 12 * steps * tokens * cols,
        ),
    )(near, queries, *sources)


def slot_place(place, core, slot):
    if slot == 0:
        return place
    if slot == 3:
        return place ^ 2
    near = place ^ 1
    far = (place + 2 * (place & 1) - 1) & (SIDE - 1)
    return jnp.where(core == slot - 1, near, far)


def placed_blocks(place_ref, shard, pieces, wanted):
    core = place_ref[0]
    where = {"z": 1, "y": 2, "x": 3}
    found = []
    for colour, orders in enumerate(ORDERS):
        unit = UNITS[colour]
        parts = []
        for level in range(3):
            first, second = orders[0][level], orders[1][level]
            place = jnp.where(core == 0, place_ref[where[first]], place_ref[where[second]])
            stride = jnp.where(core == 0, STRIDES[first], STRIDES[second])
            parts.append([slot_place(place, core, slot) * stride for slot in range(SIDE)])
        for slot in wanted:
            refs = pieces[colour][slot - wanted[0]]
            count = SIDE * SIDE // len(refs)
            for at in range(SIDE * SIDE):
                tile = parts[2][slot] + parts[1][at // SIDE] + parts[0][at % SIDE]
                target = pl.multiple_of(tile * shard + sum(UNITS[:colour]), 8)
                found.append((refs[at // count], at % count * unit, unit, target))
    return found


def start_placing(blocks, w_ref, sem):
    for ref, row, rows, target in blocks:
        pltpu.make_async_copy(ref.at[pl.ds(row, rows)], w_ref.at[pl.ds(target, rows)], sem).start()


def in_hbm(values):
    return [pltpu.with_memory_space_constraint(value, pltpu.HBM) for value in values]


def place_early(place, pieces, width, shard):
    flat = [piece for colour in pieces for piece in colour[: SIDE - 1]]
    rows, cols = sum(piece.shape[0] for piece in flat), flat[0].shape[1]

    def kernel(place_ref, *refs):
        sources, w_ref, sem = refs[:-2], refs[-2], refs[-1]
        by_colour = [[[ref] for ref in sources[: SIDE - 1]], [[ref] for ref in sources[SIDE - 1 :]]]
        start_placing(placed_blocks(place_ref, shard, by_colour, range(SIDE - 1)), w_ref, sem)
        pltpu.make_async_copy(w_ref.at[pl.ds(0, rows)], w_ref.at[pl.ds(0, rows)], sem).wait()

    return pl.pallas_call(
        kernel,
        in_specs=[pl.BlockSpec(memory_space=pltpu.SMEM)] + [pl.BlockSpec(memory_space=pltpu.HBM)] * len(flat),
        out_specs=pl.BlockSpec(memory_space=pltpu.VMEM),
        out_shape=jax.ShapeDtypeStruct((width, cols), BF16),
        scratch_shapes=[pltpu.SemaphoreType.DMA],
        compiler_params=limit(2),
        cost_estimate=pl.CostEstimate(flops=OUTPUT_COST // 4, transcendentals=0, bytes_accessed=4 * width * cols),
    )(place, *in_hbm(flat))


def multiply_into(a_ref, w_ref, out_ref, first):
    steps, tokens, cols = a_ref.shape
    left = a_ref[...].reshape(steps * tokens, cols)
    chunk = 512
    for at in range(0, out_ref.shape[2], chunk):
        right = w_ref[first + at : first + at + chunk, :]
        done = lax.dot_general(left, right, (((1,), (1,)), ((), ())), preferred_element_type=F32).astype(BF16)
        for s in range(steps):
            out_ref[1 - s, :, at : at + chunk] = done[s * tokens : (s + 1) * tokens]


def output_first(place, attended, w, pieces, shard):
    steps, tokens, cols = attended.shape
    width = w.shape[0]
    flat = [piece for colour in pieces for piece in colour[SIDE - 1 :]]
    counts = [len(colour) - SIDE + 1 for colour in pieces]
    rows = sum(piece.shape[0] for piece in flat)

    def kernel(place_ref, a_ref, w_in_ref, *refs):
        sources, out_ref, w_ref, sem = refs[:-3], refs[-3], refs[-2], refs[-1]
        by_colour = [[sources[: counts[0]]], [sources[counts[0] :]]]
        start_placing(placed_blocks(place_ref, shard, by_colour, range(SIDE - 1, SIDE)), w_ref, sem)
        pltpu.make_async_copy(w_ref.at[pl.ds(0, rows)], w_ref.at[pl.ds(0, rows)], sem).wait()
        multiply_into(a_ref, w_ref, out_ref, 0)

    return pl.pallas_call(
        kernel,
        in_specs=[pl.BlockSpec(memory_space=pltpu.SMEM)]
        + [pl.BlockSpec(memory_space=pltpu.VMEM)] * 2
        + [pl.BlockSpec(memory_space=pltpu.HBM)] * len(flat),
        out_specs=[pl.BlockSpec(memory_space=pltpu.VMEM)] * 2,
        out_shape=[
            jax.ShapeDtypeStruct((steps, tokens, width // 2), BF16),
            jax.ShapeDtypeStruct((width, cols), BF16),
        ],
        input_output_aliases={2: 1},
        scratch_shapes=[pltpu.SemaphoreType.DMA],
        compiler_params=limit(6),
        cost_estimate=pl.CostEstimate(flops=OUTPUT_COST, transcendentals=0, bytes_accessed=2 * cols * width),
    )(place, attended, w, *in_hbm(flat))


def output_second(attended, w):
    steps, tokens, cols = attended.shape
    width = w.shape[0]

    def kernel(a_ref, w_ref, out_ref):
        multiply_into(a_ref, w_ref, out_ref, width // 2)

    return pl.pallas_call(
        kernel,
        in_specs=[pl.BlockSpec(memory_space=pltpu.VMEM)] * 2,
        out_specs=pl.BlockSpec(memory_space=pltpu.VMEM),
        out_shape=jax.ShapeDtypeStruct((steps, tokens, width // 2), BF16),
        compiler_params=limit(6),
        cost_estimate=pl.CostEstimate(
            flops=steps * tokens * cols * width, transcendentals=0, bytes_accessed=cols * width
        ),
    )(attended, w)


def make_finish_kernel(parts, first):
    def kernel(
        place_ref, converged_ref, terms_ref, arrived_ref, start_ref, cached_ref, gate_ref, held_ref, pace_ref, *refs
    ):
        updated_ref, velocity_ref, buf_ref, sems = refs[-4:]
        frozen = converged_ref[place_ref[0]] > 0
        frozen_first = converged_ref[0] > 0
        rows, cols = buf_ref.shape[2:]
        span = slice(first, first + cols)
        gate = gate_ref[:, span]
        pace = pace_ref[:, span]
        copies = []
        for i in range(parts):
            at = slice(i * rows, (i + 1) * rows)
            mine = terms_ref[1, at, :].astype(F32) + arrived_ref[0, at, :].astype(F32)
            buf_ref[i, 1] = jnp.where(frozen, cached_ref[at, span], gate * mine)
            theirs = terms_ref[0, at, :].astype(F32) + arrived_ref[1, at, :].astype(F32)
            prefix = jnp.where(frozen_first, held_ref[at, span].astype(F32), pace * theirs)
            buf_ref[i, 0] = start_ref[at, span] + prefix
            for j, ref in enumerate((updated_ref, velocity_ref)):
                target = ref.at[pl.ds(i * rows, rows), pl.ds(first, cols)]
                copy = pltpu.make_async_copy(buf_ref.at[i, j], target, sems.at[i, j])
                copy.start()
                copies.append(copy)
        for copy in copies:
            copy.wait()

    return kernel


def finish(place, converged, terms, arrived, start, cached, gate, held, pace, first, so_far):
    tokens, width = start.shape
    parts, cols = 4, terms.shape[2]
    out = jax.ShapeDtypeStruct((tokens, width), F32)
    return pl.pallas_call(
        make_finish_kernel(parts, first),
        in_specs=[pl.BlockSpec(memory_space=pltpu.SMEM)] * 2
        + [pl.BlockSpec(memory_space=pltpu.VMEM)] * 7
        + [pl.BlockSpec(memory_space=pltpu.HBM)] * len(so_far),
        out_specs=[pl.BlockSpec(memory_space=pltpu.HBM)] * 2,
        out_shape=[out, out],
        input_output_aliases={9 + i: i for i in range(len(so_far))},
        scratch_shapes=[
            pltpu.VMEM((parts, 2, tokens // parts, cols), F32),
            pltpu.SemaphoreType.DMA((parts, 2)),
        ],
        compiler_params=limit(8),
        cost_estimate=pl.CostEstimate(
            flops=8 * tokens * cols, transcendentals=0, bytes_accessed=26 * tokens * cols
        ),
    )(place, converged, terms, arrived, start, cached, gate, held, pace, *so_far)


def start_gather(w_out):
    dims = tuple(order[0] for order in ORDERS[0])
    block = w_out.T[None]
    block = four(block, dims)
    parts, at = [], 0
    for unit in UNITS:
        parts.append(block[:, at : at + unit].reshape(SIDE * unit, -1))
        at += unit
    return parts


def finish_gather(colour, line):
    orders = ORDERS["ab".index(colour)]
    dims = tuple(order[1] for order in orders)
    plane = four(line, dims)
    dims = tuple(order[2] for order in orders)
    first, second = along(plane, dims, 0), along(plane, dims, 1)
    if colour == "a":
        return [plane, first, second, along(first, dims, 1)]
    half = plane.shape[0] // 2
    low = along(first[:half], dims, 1)
    return [plane, first, second, low, along(second[half:], dims, 0)]


def body(
    latents,
    start,
    cached_velocity,
    shift,
    scale,
    gate,
    step_sizes,
    converged,
    neighbours,
    w_qkv,
    q_gain,
    k_gain,
    w_out,
):
    _, width = latents.shape[1:]
    head = q_gain.shape[0]
    shard = w_out.shape[1]
    here = lax.axis_index("step")
    tile = lax.axis_index("tile")
    place = jnp.stack([here, tile // 16, tile // 4 % 4, tile % 4]).astype(jnp.int32)

    own = normalize(latents[0], scale, shift)
    other = lax.ppermute(own, "step", SWAP)

    lines = start_gather(w_out)
    pieces = [finish_gather("a", lines[0]), finish_gather("b", lines[1])]

    pair = project(own, other, w_qkv, k_gain[None], 1, 2, 1)
    around = []
    for move in (1, -1, GRID_COLS, -GRID_COLS):
        around.append(lax.ppermute(pair, "tile", neighbour_pairs(move)))
    step_size = step_sizes[0]
    to_send = (step_size * cached_velocity[0]).astype(BF16)
    sent_cached = lax.ppermute(to_send, "step", [(0, 1)])
    sent_gate = lax.ppermute(step_size * gate, "step", [(0, 1)])
    queries = project(own, other, w_qkv, q_gain[None], 0, 1, 1)
    queries, sent_cached, sent_gate = lax.optimization_barrier((queries, sent_cached, sent_gate))
    attended = attention(neighbours, queries, [pair] + around, head)
    w_placed = place_early(place, pieces, width, shard)
    left, w_placed = output_first(place, attended, w_placed, pieces, shard)
    left_arrived = lax.ppermute(left, "step", SWAP)
    right = output_second(attended, w_placed)
    right_arrived = lax.ppermute(right, "step", SWAP)
    rest = (start, cached_velocity[0], gate, sent_cached, sent_gate)
    outs = finish(place, converged[:, 0], left, left_arrived, *rest, 0, ())
    updated, velocity = finish(place, converged[:, 0], right, right_arrived, *rest, width // 2, tuple(outs))
    return (updated[None], velocity[None])


def solution(mesh):
    placed = (
        P("step", "tile", None),
        P("tile", None),
        P("step", "tile", None),
        P("step", None),
        P("step", None),
        P("step", None),
        P("step"),
        P(None, "tile"),
        P("tile", None),
        P(None, None, "step"),
        P(),
        P(),
        P("step", "tile"),
    )

    return jax.shard_map(
        body,
        mesh=mesh,
        in_specs=placed,
        out_specs=(P("step", "tile", None), P("step", "tile", None)),
        check_vma=False,
    )
```
